128 devices in a mesh: enc: 32 (over z, x, core), llm: 4 (over y).
Axes of the slice: x: 4, y: 4, z: 4, core: 2. Of those that a mesh axis runs over, the one named last changes fastest.
Arguments:
- patches: bfloat16 [16384, 5120], P('enc', 'llm'), may hold values from -6 to 6
- ln_gain: bfloat16 [1280], replicated, may hold values from 0.099609375 to 1.8984375
- w_in: bfloat16 [5120, 5120], P(None, 'llm'), may hold values from -0.078125 to 0.078125
- b_in: bfloat16 [5120], P('llm'), may hold values from -3 to 3
- w_out: bfloat16 [5120, 2048], P('llm'), may hold values from -0.078125 to 0.078125
- b_out: bfloat16 [2048], replicated, may hold values from -3 to 3
- owner: int32 [16384, 1], P(('enc', 'llm')), may hold values from 0 to 127; in each aligned block of 128 rows (0 to 127, 128 to 255, ...) at most 2 rows name the same one
- cotangent: bfloat16 [32768, 2048], P(('enc', 'llm')), may hold values from -6 to 6
Outputs:
- image_embeds: bfloat16 [32768, 2048], P(('enc', 'llm'))
- grad_w_in: float32 [5120, 5120], P('enc', 'llm')
- grad_w_out: float32 [5120, 2048], P('llm', 'enc')
- grad_patches: bfloat16 [16384, 5120], P('enc', 'llm')
The draws below stay inside these ranges and needn't reach their ends.
Inputs may be any that keep to these rules, and one draw needn't show every extreme that they name: Among the 128 consecutive tokens of one aligned block, no owner is named more than 2 times, a bound that some block reaches.
All inputs are finite; a program needn't handle non-finite values.
Results may differ from the reference program's by a relative error of at most 0.018.
Values may be sent and summed in bfloat16 or wider, within the bound.
No kernel may reach another device: no remote copies, remote signals or barrier semaphores. Data moves between devices by JAX's collectives and lax.ppermute only.
A program may use at most 192 MiB of HBM per device.

```python
import math
import jax
import jax.numpy as jnp
import numpy as np
from jax import lax

VD = 1280
OD = 2048
MERGE = 4
TOK_ENC = 512
MH = 5120
TOKENS = 16384
CAP = 2
SLOTS = 256
N_ENC = 32
N_LLM = 4
DEVICES = 128


def spiked(entries, own_key, source, target, parts, factor):
    def block_of(axis_at):
        return (jnp.arange(entries.shape[axis_at]) // (entries.shape[axis_at] // parts)).reshape((-1,) + (1,) * (entries.ndim - 1 - axis_at))

    first = jax.random.permutation(own_key, parts)[block_of(target)]
    far = (block_of(target) + parts // 2) % parts
    return jnp.where((block_of(source) == first) | (block_of(source) == far), factor * entries, entries)


def block_levels(own_key, extent, split, low, high):
    loudness, own = 1.0, jax.random.fold_in(own_key, 6)
    for position, blocks in split:
        draws = jnp.exp(jax.random.uniform(jax.random.fold_in(own, position), (blocks,), jnp.float32, low / len(split), high / len(split)))
        loudness = loudness * jnp.repeat(draws, extent[position] // blocks).reshape([-1 if axis == position else 1 for axis in range(len(extent))])
    return loudness


def routed_block(key, own, number, rows, amount, top, bound, slope):
    ranking = jax.random.permutation(key, amount)
    heavy_load, ordinary = load_shares(amount, rows * top, bound, slope, True), load_shares(amount, rows * top, bound, slope, False)
    places = jnp.arange(amount)

    def named(lengths, offset_by):
        used = int((lengths > 0).sum())
        fixed = max(1, used // 4)
        shifted = fixed + (places - fixed + offset_by * (used - fixed)) % max(1, amount - fixed)
        return jnp.zeros((amount,), jnp.int32).at[ranking[jnp.where(places < fixed, places, shifted)]].set(jnp.asarray(lengths, jnp.int32))

    lengths = jnp.where(number % 4 == 0, named(heavy_load, number // 4), named(ordinary, number - number // 4 - 1))
    mixed = jax.random.permutation(jax.random.fold_in(own, 3), amount)
    giver, receiver = mixed[0:amount // 2 * 2:2], mixed[1:amount // 2 * 2:2]
    margin = jnp.minimum(lengths[giver] - 1, bound - lengths[receiver]) // 2
    margin = jnp.where((giver == ranking[0]) | (receiver == ranking[0]) | (lengths[receiver] == 0), 0, jnp.maximum(margin, 0))
    shifted = jax.random.randint(jax.random.fold_in(own, 4), (amount // 2,), 0, 1 << 20) % (margin + 1)
    lengths = lengths.at[giver].add(-shifted).at[receiver].add(shifted)
    members = jnp.searchsorted(jnp.cumsum(lengths), jnp.arange(rows * top), side="right").astype(jnp.int32)
    table = members.reshape(top, rows).T
    table = table[jax.random.permutation(jax.random.fold_in(own, 1), rows)]
    offset_by = jax.random.randint(jax.random.fold_in(own, 2), (rows, 1), 0, top)
    return jnp.take_along_axis(table, (jnp.arange(top)[None, :] + offset_by) % top, axis=1)


def load_shares(count, total, limit, slope, full):
    weights = [(1 << 20) // math.isqrt(rank ** slope) + 1 for rank in range(1, count + 1)]
    largest = limit if full else min(limit, max(-(-total // count), total * weights[0] // sum(weights)))
    least = 1 if total - largest >= count - 1 else 0
    counts, spare = [largest] + [least] * (count - 1), total - largest - least * (count - 1)
    while spare > 0:
        movable = [i for i in range(1, count) if counts[i] < largest] or [i for i in range(1, count) if counts[i] < limit]
        whole, remaining = sum([weights[i] for i in movable]), spare
        for i in movable:
            addition = min(limit - counts[i], max(1, remaining * weights[i] // whole), spare)
            counts[i] = counts[i] + addition
            spare = spare - addition
    return np.array(counts)


def centred(key, extent, spread, reach, split=(), kind=jnp.bfloat16):
    gain = block_levels(key, extent, split, -0.22, 0.18) if split else 1.0
    result = jax.random.normal(key, extent, jnp.float32) * spread * gain
    return jnp.minimum(jnp.maximum(result, -reach), reach).astype(kind)


def heavy_noise(rng, shape, width, most, cuts, heavy, kind=jnp.bfloat16):
    drawn = width * jax.random.normal(rng, shape, jnp.float32)
    if cuts:
        drawn = drawn * block_levels(rng, shape, cuts, -0.22, 0.18)
    return jnp.clip(spiked(drawn, jax.random.fold_in(rng, 3), *heavy), -most, most).astype(kind)


def setup_inputs(seed: int = 0) -> dict:
    splits = jax.random.split(jax.random.key(seed), 9)
    patches = heavy_noise(splits[0], (TOKENS, MH), 1.0, 6.0, ((0, 32), (1, 4)), (0, 1, 32, 2.75))
    ln_gain = jnp.clip(1.0 + 0.18 * jax.random.normal(splits[1], (VD,), jnp.float32), 0.099609375, 1.8984375).astype(jnp.bfloat16)
    w_in = centred(splits[2], (MH, MH), MH ** -0.5, 0.078125, ((1, 4),))
    b_in = centred(splits[3], (MH,), 0.5, 3.0, ((0, 4),))
    w_out = centred(splits[4], (MH, OD), MH ** -0.5, 0.078125, ((0, 4),))
    b_out = centred(splits[5], (OD,), 0.5, 3.0)
    owner_keys = jax.random.split(jax.random.fold_in(splits[6], 1), TOKENS // (TOKENS // DEVICES))
    owner_turns = jax.random.permutation(jax.random.fold_in(splits[6], 3), TOKENS // (TOKENS // DEVICES))
    owner = jax.vmap(lambda own, number: routed_block(jax.random.fold_in(splits[6], 2), own, number, TOKENS // DEVICES, DEVICES, 1, CAP, 2))(owner_keys, owner_turns).reshape((TOKENS, 1))
    cotangent = centred(splits[7], (DEVICES * SLOTS, OD), 1.0, 6.0, ((0, 128),))
    return {"patches": patches, "ln_gain": ln_gain, "w_in": w_in, "b_in": b_in, "w_out": w_out, "b_out": b_out, "owner": owner, "cotangent": cotangent}


EPSILON = 1e-06
HALF_ROOT = 0.7071067811865476
DENSITY = 0.3989422804014327

def gelu_slope(hidden):
    cdf = 0.5 * (1.0 + lax.erf(hidden * HALF_ROOT))
    return cdf + hidden * jnp.exp(-0.5 * hidden * hidden) * DENSITY

def reference(patches, ln_gain, w_in, b_in, w_out, b_out, owner, cotangent):
    devices = N_ENC * N_LLM
    own_rows = TOK_ENC // N_LLM
    merged = patches.astype(jnp.float32).reshape(TOKENS, MERGE, VD)
    inverse = lax.rsqrt(lax.optimization_barrier(jnp.mean(merged * merged, axis=-1, keepdims=True)) + EPSILON)
    normed = (merged * inverse * ln_gain.astype(jnp.float32)).reshape(TOKENS, MH).astype(jnp.bfloat16)
    hidden = jnp.dot(normed, w_in, preferred_element_type=jnp.float32) + b_in.astype(jnp.float32)
    active = jax.nn.gelu(hidden, approximate=False).astype(jnp.bfloat16)
    embeds = (jnp.dot(active, w_out, preferred_element_type=jnp.float32) + b_out.astype(jnp.float32)).astype(jnp.bfloat16)
    targets = owner[:, 0].astype(jnp.int32).reshape(devices, own_rows)
    before = jnp.arange(own_rows)[:, None] > jnp.arange(own_rows)[None, :]
    same_owner = targets[:, :, None] == targets[:, None, :]
    rank_in = lax.optimization_barrier(jnp.sum(jnp.logical_and(same_owner, before[None]), axis=2)).astype(jnp.int32)
    sources = jnp.arange(devices, dtype=jnp.int32)[:, None]
    slot_ids = (targets * (devices * CAP) + sources * CAP + rank_in).reshape(TOKENS).astype(jnp.int32)
    image_embeds = jnp.zeros((devices * devices * CAP, OD), jnp.bfloat16).at[slot_ids].set(embeds)
    grad_embeds = cotangent[slot_ids]
    grad_active = jnp.dot(grad_embeds, w_out.T, preferred_element_type=jnp.float32)
    grad_hidden = (grad_active * gelu_slope(hidden)).astype(jnp.bfloat16)

    def add_group(carry, items):
        normed_part, active_part, hidden_part, embeds_part = items
        in_part = jnp.dot(normed_part.T, hidden_part, preferred_element_type=jnp.float32).astype(jnp.bfloat16)
        out_part = jnp.dot(active_part.T, embeds_part, preferred_element_type=jnp.float32).astype(jnp.bfloat16)
        in_part, out_part = lax.optimization_barrier((in_part, out_part))
        return ((carry[0] + in_part.astype(jnp.float32), carry[1] + out_part.astype(jnp.float32)), None)
    zero_init = (jnp.zeros((MH, MH), jnp.float32), jnp.zeros((MH, OD), jnp.float32))
    items = (normed.reshape(N_ENC, TOK_ENC, MH), active.reshape(N_ENC, TOK_ENC, MH), grad_hidden.reshape(N_ENC, TOK_ENC, MH), grad_embeds.reshape(N_ENC, TOK_ENC, OD))
    (grad_w_in, grad_w_out), unused = lax.scan(add_group, zero_init, items)
    grad_normed = jnp.dot(grad_hidden, w_in.T, preferred_element_type=jnp.float32)
    scaled = grad_normed.reshape(TOKENS, MERGE, VD) * ln_gain.astype(jnp.float32)
    projection = lax.optimization_barrier(jnp.mean(scaled * merged, axis=-1, keepdims=True))
    cubed = inverse * inverse * inverse
    grad_patches = (inverse * scaled - merged * cubed * projection).reshape(TOKENS, MH).astype(jnp.bfloat16)
    return (image_embeds, grad_w_in, grad_w_out, grad_patches)
```

```python
import jax
import jax.numpy as jnp
from jax import lax
from jax.sharding import Mesh
from jax.sharding import PartitionSpec as P

EPSILON = 1e-06
HALF_ROOT = 0.7071067811865476
DENSITY = 0.3989422804014327
RING = 4
BF = jnp.bfloat16
F32 = jnp.float32


def send(value, axis, step):
    return lax.ppermute(value, axis, [(i, (i + step) % RING) for i in range(RING)])


def swap(value):
    return lax.ppermute(value, "c", [(0, 1), (1, 0)])


def pick(stacked, index):
    return lax.dynamic_index_in_dim(stacked, index, 0, keepdims=False)


def gather_ring(own, axis):
    half = own.shape[0] // 2
    before = send(own, axis, 1)
    after = send(own, axis, -1)
    far_low = send(before[:half], axis, 1)
    far_high = send(after[half:], axis, -1)
    return own, after, jnp.concatenate([far_low, far_high], axis=0), before


def add_into(chunk, low=None, high=None):
    half = chunk.shape[0] // 2
    first, second = chunk[:half], chunk[half:]
    if low is not None:
        first = (first.astype(F32) + low.astype(F32)).astype(BF)
    if high is not None:
        second = (second.astype(F32) + high.astype(F32)).astype(BF)
    return jnp.concatenate([first, second], axis=0)


def reduce_ring(chunk, axis):
    far = chunk(2)
    half = far.shape[0] // 2
    low = send(far[:half], axis, 1)
    high = send(far[half:], axis, -1)
    from_before = send(add_into(chunk(1), low=low), axis, 1)
    from_after = send(add_into(chunk(3), high=high), axis, -1)
    return chunk(0).astype(F32) + from_before.astype(F32) + from_after.astype(F32)


def reduce_torus(terms):
    x = lax.axis_index("x")
    stacked = jnp.stack(terms)
    by_x = jnp.moveaxis(stacked[:, :, 0], 1, 0)
    first = reduce_ring(lambda k: pick(by_x, (x + k) % RING), "x").astype(BF)
    second = reduce_ring(lambda j: terms[j][:, 1], "z").astype(BF)
    low = reduce_ring(lambda j: first[j], "z").astype(BF)
    high = reduce_ring(lambda k: pick(second, (x + k) % RING), "x").astype(BF)
    core = lax.axis_index("c")
    other = swap(jnp.where(core == 0, high, low))
    own = jnp.where(core == 0, low, high)
    return jnp.where(
        core == 0,
        jnp.concatenate([own, other], axis=1),
        jnp.concatenate([other, own], axis=1),
    ).astype(F32)


def t_dot(left, right):
    return lax.dot_general(left, right, (((0,), (0,)), ((), ())), preferred_element_type=F32)


def dot_t(left, right):
    return lax.dot_general(left, right, (((1,), (1,)), ((), ())), preferred_element_type=F32)


def local(patches, ln_gain, w_in, b_in, w_out, b_out, owner, cotangent):
    z, x, core, y = (lax.axis_index(name) for name in ("z", "x", "c", "y"))
    everyone = ("z", "x", "c", "y")
    devices = lax.axis_size(everyone)
    slot_cap = cotangent.shape[0] // devices
    tokens, width = patches.shape
    gain = ln_gain.astype(F32)
    merged = patches.astype(F32)
    inverse = lax.rsqrt(jnp.mean(merged * merged, axis=-1, keepdims=True) + EPSILON)
    own_normed = (merged * inverse * gain).astype(BF)
    normed = gather_ring(own_normed, "y")
    returned = lax.all_to_all(cotangent, everyone, split_axis=0, concat_axis=0, tiled=True)

    own_rows = tokens // RING
    targets = owner[:, 0]
    before = jnp.arange(own_rows)[:, None] > jnp.arange(own_rows)[None, :]
    same_owner = targets[:, None] == targets[None, :]
    rank_in = jnp.sum(jnp.logical_and(same_owner, before), axis=1)
    slot_ids = targets * slot_cap + rank_in
    placing = (
        jnp.arange(devices * slot_cap, dtype=jnp.int32)[:, None] == slot_ids[None, :]
    ).astype(BF)

    own_grad = t_dot(placing, returned).astype(BF)
    grad_parts = gather_ring(own_grad, "y")
    grad_embeds = jnp.zeros((RING, *own_grad.shape), BF)
    for k, part in enumerate(grad_parts):
        grad_embeds = lax.dynamic_update_index_in_dim(grad_embeds, part, (y + k) % RING, 0)
    grad_embeds = grad_embeds.reshape(tokens, -1)

    w_in_blocks = w_in.reshape(RING, width, -1)
    hidden = b_in.astype(F32)
    for k in (0, 1, 3, 2):
        hidden = hidden + jnp.dot(
            normed[k], pick(w_in_blocks, (y + k) % RING), preferred_element_type=F32
        )
    cdf = 0.5 * (1.0 + lax.erf(hidden * HALF_ROOT))
    active = (hidden * cdf).astype(BF)
    slope = cdf + hidden * jnp.exp(-0.5 * hidden * hidden) * DENSITY

    grad_hidden = (dot_t(grad_embeds, w_out) * slope).astype(BF)
    half = grad_hidden.shape[1] // 2

    def own_half(value):
        return lax.dynamic_slice_in_dim(value, core * half, half, 1)

    def other_half(value):
        return lax.dynamic_slice_in_dim(value, (1 - core) * half, half, 1)

    def pair(value):
        return jnp.concatenate([own_half(value), swap(other_half(value))], axis=0)

    partial = jnp.dot(active, w_out, preferred_element_type=F32).astype(BF)
    partial = partial.reshape(RING, own_rows, -1)
    summed = reduce_ring(lambda k: pick(partial, (y + k) % RING), "y")
    embeds = (summed + b_out.astype(F32)).astype(BF)
    outgoing = jnp.dot(placing, embeds, preferred_element_type=F32).astype(BF)
    image_embeds = lax.all_to_all(outgoing, everyone, split_axis=0, concat_axis=0, tiled=True)

    def feature_term(k):
        return dot_t(grad_hidden, pick(w_in_blocks, (y + k) % RING)).astype(BF)

    grad_normed = reduce_ring(feature_term, "y")
    scaled = grad_normed * gain
    projection = jnp.mean(scaled * merged, axis=-1, keepdims=True)
    cubed = inverse * inverse * inverse
    grad_patches = (inverse * scaled - merged * cubed * projection).astype(BF)

    pair_embeds = jnp.concatenate([grad_embeds, swap(grad_embeds)], axis=0)
    out_term = t_dot(pair_embeds, pair(active)).astype(BF)
    out_term = out_term.reshape(RING, RING, 2, -1, half)
    grad_w_out = reduce_torus([pick(out_term, (z + j) % RING) for j in range(RING)]).T

    pair_normed = jnp.stack([jnp.concatenate([part, swap(part)], axis=0) for part in normed])
    pair_hidden = pair(grad_hidden)

    def in_term(j):
        term = t_dot(pick(pair_normed, (z + j - y) % RING), pair_hidden).astype(BF)
        return term.reshape(RING, 2, -1, half)

    grad_w_in = reduce_torus([in_term(j) for j in range(RING)])
    return (image_embeds, grad_w_in, grad_w_out, grad_patches)


def solution(mesh):
    grid = Mesh(mesh.devices.reshape(RING, RING, 2, RING), ("z", "x", "c", "y"))
    enc = ("z", "x", "c")
    everyone = (*enc, "y")
    in_specs = (
        P(enc, "y"),
        P(),
        P(None, "y"),
        P("y"),
        P("y", None),
        P(),
        P(everyone, None),
        P(everyone, None),
    )
    out_specs = (P(everyone, None), P(enc, "y"), P("y", enc), P(enc, "y"))
    return jax.shard_map(
        local, mesh=grid, in_specs=in_specs, out_specs=out_specs, check_vma=False
    )
```

```python
import jax
import jax.numpy as jnp
from jax import lax
from jax.experimental import pallas as pl
from jax.experimental.pallas import tpu as pltpu
from jax.sharding import Mesh
from jax.sharding import PartitionSpec as P


EPSILON = 1e-06
HALF_ROOT = 0.7071067811865476
DENSITY = 0.3989422804014327
RING = 4
BF = jnp.bfloat16
F32 = jnp.float32


def send(value, axis, reverse=False):
    pairs = []
    for place in range(RING):
        for core in range(2):
            to = (place + (1 - 2 * core) * (-1 if reverse else 1)) % RING
            if axis == "y":
                pairs.append((core * RING + place, core * RING + to))
            else:
                pairs.append((2 * place + core, 2 * to + core))
    return lax.ppermute(value, ("c", "y") if axis == "y" else (axis, "c"), pairs)


def send_across(value, axis):
    return lax.ppermute(value, axis, [(i, (i + 2) % RING) for i in range(RING)])


def swap(value):
    return lax.ppermute(value, "c", [(0, 1), (1, 0)])


def exchange(value, axis):
    return lax.all_to_all(value, axis, 0, 0, tiled=True)


def pick(stacked, index):
    return lax.dynamic_index_in_dim(stacked, index, 0, keepdims=False)


def t_dot(left, right):
    return lax.dot_general(left, right, (((0,), (0,)), ((), ())), preferred_element_type=F32)


def dot_t(left, right):
    return lax.dot_general(left, right, (((1,), (1,)), ((), ())), preferred_element_type=F32)


def plus(first, second):
    return first.astype(F32) + second.astype(F32)


def total(pieces):
    return jnp.sum(pieces.astype(F32), axis=0)


def weight_kernel(own_left, other_left, own_right, other_right, low, high):
    rows = low.shape[2]
    width = 2 * RING * rows
    own, other = (left[...].reshape(-1, width) for left in (own_left, other_left))
    term = t_dot(own, own_right[0]) + t_dot(other, other_right[...])
    for x in range(RING):
        start = 2 * rows * x
        low[x, 0] = term[start : start + rows].astype(BF)
        high[0, x] = term[start + rows : start + 2 * rows].astype(BF)


def weight_terms(own_left, other_left, own_right, other_right):
    tokens = own_left.shape[-2]
    columns = own_right.shape[2]
    if own_left.ndim == 3:
        width = own_left.shape[2]
        left = pl.BlockSpec((1, tokens, width), lambda z: (z, 0, 0))
    else:
        width = own_left.shape[1] // RING
        left = pl.BlockSpec((tokens, width), lambda z: (0, z))
    rows = width // (2 * RING)
    return pl.pallas_call(
        weight_kernel,
        grid=(RING,),
        in_specs=[
            left,
            left,
            pl.BlockSpec((1, tokens, columns), lambda z: (0, 0, 0)),
            pl.BlockSpec((tokens, columns), lambda z: (0, 0)),
        ],
        out_specs=[
            pl.BlockSpec((RING, 1, rows, columns), lambda z: (0, z, 0, 0)),
            pl.BlockSpec((1, RING, rows, columns), lambda z: (z, 0, 0, 0)),
        ],
        out_shape=[jax.ShapeDtypeStruct((RING, RING, rows, columns), BF)] * 2,
        cost_estimate=cost(4 * RING * tokens * width * columns, 20_000_000),
    )(own_left, other_left, own_right, other_right)


def cost(flops, moved):
    return pl.CostEstimate(flops=flops, bytes_accessed=moved, transcendentals=0)


def hidden_kernel(where, part, weights, held, active, slope):
    hidden = held[...] + jnp.dot(part[...], weights[0], preferred_element_type=F32)
    cdf = 0.5 * (1.0 + lax.erf(hidden * HALF_ROOT))
    active[0] = (hidden * cdf).astype(BF)
    slope[0] = cdf + hidden * jnp.exp(-0.5 * hidden * hidden) * DENSITY


def hidden_end(core, block, part, weights, held):
    tokens, width = part.shape
    half = held.shape[1] // 2
    rows = tokens // 2

    def side(i, where):
        return (i + where[0]) % 2

    out = pl.BlockSpec((1, rows, half), lambda i, r, where: (i, r, 0))
    return pl.pallas_call(
        hidden_kernel,
        grid_spec=pltpu.PrefetchScalarGridSpec(
            num_scalar_prefetch=1,
            grid=(2, 2),
            in_specs=[
                pl.BlockSpec((rows, width), lambda i, r, where: (r, 0)),
                pl.BlockSpec((1, width, half), lambda i, r, where: (where[1], 0, side(i, where))),
                pl.BlockSpec((rows, half), lambda i, r, where: (r, side(i, where))),
            ],
            out_specs=[out, out],
        ),
        out_shape=[
            jax.ShapeDtypeStruct((2, tokens, half), BF),
            jax.ShapeDtypeStruct((2, tokens, half), F32),
        ],
        cost_estimate=cost(4 * tokens * width * half, 9_000_000),
        name="hidden_end",
    )(jnp.stack([core, block]), part, weights, held)


def embeds_kernel(where, own, other, own_weights, other_weights, out):
    term = jnp.dot(own[0], own_weights[...], preferred_element_type=F32)
    term = term + jnp.dot(other[0], other_weights[...], preferred_element_type=F32)
    out[...] = term.astype(BF)


def embeds_terms(core, active, weights):
    half, columns = active.shape[2], weights.shape[1]
    tokens, cut = active.shape[1], columns // 4
    return pl.pallas_call(
        embeds_kernel,
        grid_spec=pltpu.PrefetchScalarGridSpec(
            num_scalar_prefetch=1,
            grid=(4,),
            in_specs=[
                pl.BlockSpec((1, tokens, half), lambda i, where: (0, 0, 0)),
                pl.BlockSpec((1, tokens, half), lambda i, where: (1, 0, 0)),
                pl.BlockSpec((half, cut), lambda i, where: (where[0], i)),
                pl.BlockSpec((half, cut), lambda i, where: (1 - where[0], i)),
            ],
            out_specs=pl.BlockSpec((tokens, cut), lambda i, where: (0, i)),
        ),
        out_shape=jax.ShapeDtypeStruct((tokens, columns), BF),
        cost_estimate=cost(4 * tokens * half * columns, 9_000_000),
        name="embeds_terms",
    )(jnp.stack([core, core]), active, active, weights, weights)


def grad_kernel(where, *refs):
    *parts, weights, slope, grad_hidden, grad_embeds = refs

    @pl.when(pl.program_id(0) == 0)
    def _():
        rows = parts[0].shape[0]
        for j, part in enumerate(parts):
            grad_embeds[pl.ds(pl.multiple_of(where[1 + j] * rows, rows), rows), :] = part[...]

    grad_active = dot_t(grad_embeds[...], weights[...])
    grad_hidden[0] = (grad_active * slope[0]).astype(BF)


def grad_terms(core, places, parts, weights, slope):
    tokens, half = slope.shape[1:]
    rows, columns = parts[0].shape
    whole = pl.BlockSpec((rows, columns), lambda i, where: (0, 0))
    side = pl.BlockSpec((1, tokens, half), lambda i, where: (i, 0, 0))
    return pl.pallas_call(
        grad_kernel,
        grid_spec=pltpu.PrefetchScalarGridSpec(
            num_scalar_prefetch=1,
            grid=(2,),
            in_specs=[
                *([whole] * RING),
                pl.BlockSpec((half, columns), lambda i, where: ((i + where[0]) % 2, 0)),
                side,
            ],
            out_specs=[side, pl.BlockSpec((tokens, columns), lambda i, where: (0, 0))],
        ),
        out_shape=[
            jax.ShapeDtypeStruct(slope.shape, BF),
            jax.ShapeDtypeStruct((tokens, columns), BF),
        ],
        cost_estimate=cost(4 * tokens * half * columns, 12_000_000),
        name="grad_terms",
    )(jnp.stack([core, *places]), *parts, weights, slope)


def feature_kernel(where, own, other, own_weights, other_weights, out):
    term = dot_t(own[0], own_weights[0]) + dot_t(other[0], other_weights[0])
    out[0] = term.astype(BF)


def feature_terms(core, places, grad_hidden, weights):
    tokens, half = grad_hidden.shape[1:]
    width = weights.shape[1]
    cut = width // 2
    return pl.pallas_call(
        feature_kernel,
        grid_spec=pltpu.PrefetchScalarGridSpec(
            num_scalar_prefetch=1,
            grid=(len(places), 2),
            in_specs=[
                pl.BlockSpec((1, tokens, half), lambda k, i, where: (0, 0, 0)),
                pl.BlockSpec((1, tokens, half), lambda k, i, where: (1, 0, 0)),
                pl.BlockSpec((1, cut, half), lambda k, i, where: (where[1 + k], i, where[0])),
                pl.BlockSpec((1, cut, half), lambda k, i, where: (where[1 + k], i, 1 - where[0])),
            ],
            out_specs=pl.BlockSpec((1, tokens, cut), lambda k, i, where: (k, 0, i)),
        ),
        out_shape=jax.ShapeDtypeStruct((len(places), tokens, width), BF),
        cost_estimate=cost(4 * len(places) * tokens * half * width, 6_000_000 * len(places)),
    )(jnp.stack([core, *places]), grad_hidden, grad_hidden, weights, weights)


def local(patches, ln_gain, w_in, b_in, w_out, b_out, owner, cotangent):
    z, x, core, y = (lax.axis_index(name) for name in ("z", "x", "c", "y"))
    way = 1 - 2 * core
    everyone = ("z", "x", "c", "y")
    devices = lax.axis_size(everyone)
    slot_cap = cotangent.shape[0] // devices
    tokens, width = patches.shape
    own_rows = tokens // RING
    gain = ln_gain.astype(F32)
    last = owner

    def start_pair(terms):
        return pick(terms[0], (x + way * 3) % RING), pick(terms[1], (z + way * 3) % RING)

    def send_pair(pair):
        return send(pair[0], "x"), send(pair[1], "z")

    def add_pair(terms, k, arrived):
        low = pick(terms[0], (x + way * k) % RING).astype(F32) + arrived[0].astype(F32)
        high = pick(terms[1], (z + way * k) % RING).astype(F32) + arrived[1].astype(F32)
        return low.astype(BF), high.astype(BF)

    def go(*values):
        out = lax.optimization_barrier((*values, last))[:-1]
        return out if len(out) > 1 else out[0]

    def mark(value):
        nonlocal last
        last = value
        return value

    def place(places):
        return (y + way * places) % RING

    targets = owner[:, 0]
    before = jnp.arange(own_rows)[:, None] > jnp.arange(own_rows)[None, :]
    same_owner = targets[:, None] == targets[None, :]
    rank_in = jnp.sum(jnp.logical_and(same_owner, before), axis=1)
    slot_ids = targets * slot_cap + rank_in
    placing = (
        jnp.arange(devices * slot_cap, dtype=jnp.int32)[:, None] == slot_ids[None, :]
    ).astype(BF)

    merged = patches.astype(F32)
    inverse = lax.rsqrt(jnp.mean(merged * merged, axis=-1, keepdims=True) + EPSILON)
    part = mark((merged * inverse * gain).astype(BF))
    coming = send(part, "y")
    returned = exchange(go(cotangent), everyone)

    w_in_blocks = w_in.reshape(RING, width, -1)
    normed = jnp.zeros((RING, tokens, width), BF)
    hidden = b_in.astype(F32)

    def take(j, part, normed, hidden):
        block = pick(w_in_blocks, place(-j))
        normed = lax.dynamic_update_index_in_dim(normed, part, place(-j), 0)
        return normed, hidden + jnp.dot(part, block, preferred_element_type=F32)

    normed, hidden = take(0, go(part), normed, hidden)
    mark(hidden)
    part = go(coming)
    coming = send(part, "y")
    normed, hidden = take(1, part, normed, hidden)
    mark(hidden)
    grads = [mark(t_dot(placing, go(returned)).astype(BF))]
    coming_grad = send(grads[0], "y")
    part = mark(go(coming))
    coming = send(part, "y")
    grads.append(mark(go(coming_grad)))
    coming_grad = send(grads[1], "y")
    normed, hidden = take(2, go(part), normed, hidden)
    mark(hidden)
    grads.append(mark(go(coming_grad)))
    coming_grad = send(grads[2], "y")
    part = go(coming)
    normed = lax.dynamic_update_index_in_dim(normed, part, place(-3), 0)
    other_normed = swap(normed)
    active, slope = mark(hidden_end(core, place(-3), part, w_in_blocks, hidden))
    other_active = swap(active[1])

    partial = mark(embeds_terms(core, go(active), w_out))
    pieces = exchange(partial.reshape(RING, own_rows, -1), "y")

    grads.append(go(coming_grad))
    grad_hidden, grad_embeds = mark(
        grad_terms(core, [place(-j) for j in range(RING)], grads, w_out, slope)
    )
    other_hidden = swap(grad_hidden[1])
    other_embeds = swap(grad_embeds)

    held = mark(feature_terms(core, [place(3)], go(grad_hidden), w_in_blocks)[0])
    coming = send(held, "y")

    in_terms = mark(weight_terms(*go(normed, other_normed, grad_hidden, other_hidden)))
    in_held = go(*start_pair(in_terms))
    in_coming = send_pair(in_held)

    features = mark(
        feature_terms(core, [place(k) for k in (2, 1, 0)], go(grad_hidden), w_in_blocks)
    )
    out_terms = mark(weight_terms(*go(grad_embeds, other_embeds, active, other_active)))
    out_held = go(*start_pair(out_terms))
    out_coming = send_pair(out_held)

    held = mark(plus(features[0], go(coming)).astype(BF))
    coming = send(held, "y")

    in_held = mark(add_pair(in_terms, 2, go(*in_coming)))
    in_coming = send_pair(in_held)
    out_held = mark(add_pair(out_terms, 2, go(*out_coming)))
    out_coming = send_pair(out_held)

    held = mark(plus(features[1], go(coming)).astype(BF))
    coming = send(held, "y")

    in_held = mark(add_pair(in_terms, 1, go(*in_coming)))
    in_coming = send_pair(in_held)
    out_held = mark(add_pair(out_terms, 1, go(*out_coming)))
    out_coming = send_pair(out_held)

    embeds = (total(go(pieces)) + b_out.astype(F32)).astype(BF)
    outgoing = mark(jnp.dot(placing, embeds, preferred_element_type=F32).astype(BF))
    image_embeds = exchange(outgoing, everyone)

    in_low, in_high = add_pair(in_terms, 0, go(*in_coming))
    mark(in_low)
    out_low, out_high = add_pair(out_terms, 0, go(*out_coming))
    low = jnp.concatenate([in_low, out_low], axis=1)
    high = jnp.concatenate([in_high, out_high], axis=1)
    mark((low, high))

    def term(value, index, k):
        return pick(value, (index + way * k) % RING)

    arrived_low = (
        send(term(low, z, 1), "z"),
        send_across(term(low, z, 2), "z"),
        send(term(low, z, 3), "z", reverse=True),
    )
    arrived_high = (
        send(term(high, x, 1), "x"),
        send_across(term(high, x, 2), "x"),
        send(term(high, x, 3), "x", reverse=True),
    )

    grad_normed = plus(features[2], go(coming))
    scaled = grad_normed * gain
    projection = jnp.mean(scaled * merged, axis=-1, keepdims=True)
    cubed = inverse * inverse * inverse
    grad_patches = mark((inverse * scaled - merged * cubed * projection).astype(BF))

    def whole(own, arrived):
        return sum((piece.astype(F32) for piece in arrived), own.astype(F32)).astype(BF)

    arrived_low, arrived_high = go(arrived_low, arrived_high)
    low, high = whole(pick(low, z), arrived_low), whole(pick(high, x), arrived_high)
    other = swap(jnp.where(core == 0, high, low))
    own = jnp.where(core == 0, low, high)
    rows = jnp.where(
        core == 0,
        jnp.concatenate([own, other], axis=1),
        jnp.concatenate([other, own], axis=1),
    ).astype(F32)
    split = width // (2 * RING)
    return (image_embeds, rows[:split], rows[split:].T, grad_patches)


def solution(mesh):
    grid = Mesh(mesh.devices.reshape(RING, RING, 2, RING), ("z", "x", "c", "y"))
    enc = ("z", "x", "c")
    everyone = (*enc, "y")
    in_specs = (
        P(enc, "y"),
        P(),
        P(None, "y"),
        P("y"),
        P("y", None),
        P(),
        P(everyone, None),
        P(everyone, None),
    )
    out_specs = (P(everyone, None), P(enc, "y"), P("y", enc), P(enc, "y"))

    return jax.shard_map(local, mesh=grid, in_specs=in_specs, out_specs=out_specs, check_vma=False)
```

```python
import jax
import jax.numpy as jnp
from jax import lax
from jax.experimental import pallas as pl
from jax.experimental.pallas import tpu as pltpu
from jax.sharding import Mesh
from jax.sharding import PartitionSpec as P


EPSILON = 1e-06
HALF_ROOT = 0.7071067811865476
DENSITY = 0.3989422804014327
RING = 4
BF = jnp.bfloat16
F32 = jnp.float32


def send(value, axis, reverse=False):
    pairs = []
    for place in range(RING):
        for core in range(2):
            to = (place + (1 - 2 * core) * (-1 if reverse else 1)) % RING
            if axis == "y":
                pairs.append((core * RING + place, core * RING + to))
            else:
                pairs.append((2 * place + core, 2 * to + core))
    return lax.ppermute(value, ("c", "y") if axis == "y" else (axis, "c"), pairs)


def send_across(value, axis):
    return lax.ppermute(value, axis, [(i, (i + 2) % RING) for i in range(RING)])


def swap(value):
    return lax.ppermute(value, "c", [(0, 1), (1, 0)])


def exchange(value, axis):
    return lax.all_to_all(value, axis, 0, 0, tiled=True)


def pick(stacked, index):
    return lax.dynamic_index_in_dim(stacked, index, 0, keepdims=False)


def t_dot(left, right):
    return lax.dot_general(left, right, (((0,), (0,)), ((), ())), preferred_element_type=F32)


def dot_t(left, right):
    return lax.dot_general(left, right, (((1,), (1,)), ((), ())), preferred_element_type=F32)


def plus(first, second):
    return first.astype(F32) + second.astype(F32)


def total(pieces):
    return jnp.sum(pieces.astype(F32), axis=0)


def weight_kernel(where, own_left, other_left, own_right, other_right, low, high, low_start, high_start):
    rows = low.shape[2]
    width = RING * rows

    def one(i, carry):
        cut = pl.ds(pl.multiple_of(i * width, width), width)
        own, other = (
            left[0, :, cut] if len(left.shape) == 3 else left[:, cut]
            for left in (own_left, other_left)
        )
        term = t_dot(own, own_right[...]) + t_dot(other, other_right[...])
        for x in range(2):
            start = 2 * rows * x
            low[2 * i + x, 0] = term[start : start + rows].astype(BF)
            high[0, 2 * i + x] = term[start + rows : start + 2 * rows].astype(BF)
        return carry

    lax.fori_loop(0, 2, one, 0)
    low_start[0] = low[where[0], 0]

    @pl.when(pl.program_id(0) == where[1])
    def _():
        high_start[...] = high[0]


def weight_terms(starts, own_left, other_left, own_right, other_right):
    tokens = own_left.shape[-2]
    columns = own_right.shape[1]
    if own_left.ndim == 3:
        width = own_left.shape[2]
        left = pl.BlockSpec((1, tokens, width), lambda z, where: (z, 0, 0))
    else:
        width = own_left.shape[1] // RING
        left = pl.BlockSpec((tokens, width), lambda z, where: (0, z))
    rows = width // (2 * RING)
    right = pl.BlockSpec((tokens, columns), lambda z, where: (0, 0))
    whole = jax.ShapeDtypeStruct((RING, RING, rows, columns), BF)
    first = jax.ShapeDtypeStruct((RING, rows, columns), BF)
    return pl.pallas_call(
        weight_kernel,
        grid_spec=pltpu.PrefetchScalarGridSpec(
            num_scalar_prefetch=1,
            grid=(RING,),
            in_specs=[left, left, right, right],
            out_specs=[
                pl.BlockSpec((RING, 1, rows, columns), lambda z, where: (0, z, 0, 0)),
                pl.BlockSpec((1, RING, rows, columns), lambda z, where: (z, 0, 0, 0)),
                pl.BlockSpec((1, rows, columns), lambda z, where: (z, 0, 0)),
                pl.BlockSpec((RING, rows, columns), lambda z, where: (0, 0, 0)),
            ],
        ),
        out_shape=[whole, whole, first, first],
        cost_estimate=cost(4 * RING * tokens * width * columns, 20_000_000),
    )(jnp.stack(starts), own_left, other_left, own_right, other_right)


def cost(flops, moved):
    return pl.CostEstimate(flops=flops, bytes_accessed=moved, transcendentals=0)


def local(patches, ln_gain, w_in, b_in, w_out, b_out, owner, cotangent):
    z, x, core, y = (lax.axis_index(name) for name in ("z", "x", "c", "y"))
    way = 1 - 2 * core
    everyone = ("z", "x", "c", "y")
    devices = lax.axis_size(everyone)
    slot_cap = cotangent.shape[0] // devices
    tokens, width = patches.shape
    own_rows = tokens // RING
    gain = ln_gain.astype(F32)
    last = owner

    def send_all(in_pair, out_pair):
        low, high, out_low, out_high = lax.optimization_barrier((*in_pair, *out_pair))
        return (
            (send(low, "x"), send(high, "z")),
            (send(out_low, "x"), send(out_high, "z")),
        )

    def add_pair(terms, k, arrived):
        low = pick(terms[0], (x + way * k) % RING).astype(F32) + arrived[0].astype(F32)
        high = pick(terms[1], (z + way * k) % RING).astype(F32) + arrived[1].astype(F32)
        return low.astype(BF), high.astype(BF)

    def go(*values):
        out = lax.optimization_barrier((*values, last))[:-1]
        return out if len(out) > 1 else out[0]

    def mark(value):
        nonlocal last
        last = value
        return value

    def place(places):
        return (y + way * places) % RING

    targets = owner[:, 0]
    before = jnp.arange(own_rows)[:, None] > jnp.arange(own_rows)[None, :]
    same_owner = targets[:, None] == targets[None, :]
    rank_in = jnp.sum(jnp.logical_and(same_owner, before), axis=1)
    slot_ids = targets * slot_cap + rank_in
    placing = (
        jnp.arange(devices * slot_cap, dtype=jnp.int32)[:, None] == slot_ids[None, :]
    ).astype(BF)

    merged = patches.astype(F32)
    inverse = lax.rsqrt(jnp.mean(merged * merged, axis=-1, keepdims=True) + EPSILON)
    part = mark((merged * inverse * gain).astype(BF))
    coming = send(part, "y")
    returned = exchange(go(cotangent), everyone)

    w_in_blocks = w_in.reshape(RING, width, -1)
    normed = jnp.zeros((RING, tokens, width), BF)
    hidden = b_in.astype(F32)

    def keep(j, part, normed):
        return lax.dynamic_update_index_in_dim(normed, part, place(-j), 0)

    def take(j, part, hidden):
        block = pick(w_in_blocks, place(-j))
        return hidden + jnp.dot(part, block, preferred_element_type=F32)

    normed = keep(0, part, normed)
    hidden = take(0, go(part), hidden)
    mark(hidden)
    part = go(coming)
    coming = send(part, "y")
    normed = keep(1, part, normed)
    hidden = take(1, part, hidden)
    mark(hidden)
    part_grad = mark(t_dot(placing, go(returned)).astype(BF))
    coming_grad = send(part_grad, "y")
    grad_embeds = jnp.zeros((RING, *part_grad.shape), BF)
    grad_embeds = lax.dynamic_update_index_in_dim(grad_embeds, part_grad, y, 0)
    part = mark(go(coming))
    coming = send(part, "y")
    normed = mark(keep(2, part, normed))
    part_grad = mark(go(coming_grad))
    coming_grad = send(part_grad, "y")
    grad_embeds = lax.dynamic_update_index_in_dim(grad_embeds, part_grad, place(-1), 0)
    hidden = mark(take(2, go(part), hidden))
    part_grad = mark(go(coming_grad))
    coming_grad = send(part_grad, "y")
    grad_embeds = lax.dynamic_update_index_in_dim(grad_embeds, part_grad, place(-2), 0)
    mark(grad_embeds)
    part = go(coming)
    normed = keep(3, part, normed)
    hidden = take(3, part, hidden)
    other_normed = swap(normed)
    cdf = 0.5 * (1.0 + lax.erf(hidden * HALF_ROOT))
    active = mark((hidden * cdf).astype(BF))
    slope = cdf + hidden * jnp.exp(-0.5 * hidden * hidden) * DENSITY

    half = active.shape[1] // 2

    def own_half(value, which):
        return lax.dynamic_slice_in_dim(value, which * half, half, 1)

    partial = mark(jnp.dot(go(active), w_out, preferred_element_type=F32).astype(BF))
    pieces = exchange(partial.reshape(RING, own_rows, -1), "y")

    grad_embeds = lax.dynamic_update_index_in_dim(grad_embeds, go(coming_grad), place(-3), 0)
    grad_embeds = grad_embeds.reshape(tokens, -1)
    other_embeds = swap(grad_embeds)
    grad_hidden = mark((dot_t(grad_embeds, w_out) * slope).astype(BF))
    own_hidden, own_active = own_half(grad_hidden, core), own_half(active, core)
    other_hidden = swap(own_half(grad_hidden, 1 - core))
    other_active = swap(own_half(active, 1 - core))

    def feature_term(k, hidden_now):
        return dot_t(hidden_now, pick(w_in_blocks, place(k))).astype(BF)

    held = mark(feature_term(3, go(grad_hidden)))
    coming = send(held, "y")

    hidden_now = go(grad_hidden)
    features = mark([feature_term(k, hidden_now) for k in (2, 1, 0)])

    starts = [(x + way * 3) % RING, (z + way * 3) % RING]
    *out_terms, low, high = mark(
        weight_terms(starts, *go(grad_embeds, other_embeds, own_active, other_active))
    )
    out_held = low, high
    *in_terms, low, high = mark(
        weight_terms(starts, *go(normed, other_normed, own_hidden, other_hidden))
    )
    in_coming, out_coming = send_all((low, high), out_held)
    held = mark(plus(features[0], go(coming)).astype(BF))

    coming = send(held, "y")
    in_held = mark(add_pair(in_terms, 2, go(*in_coming)))
    out_held = mark(add_pair(out_terms, 2, go(*out_coming)))
    in_coming, out_coming = send_all(in_held, out_held)

    held = mark(plus(features[1], go(coming)).astype(BF))
    coming = send(held, "y")

    in_held = mark(add_pair(in_terms, 1, go(*in_coming)))
    out_held = mark(add_pair(out_terms, 1, go(*out_coming)))
    in_coming, out_coming = send_all(in_held, out_held)

    embeds = (total(go(pieces)) + b_out.astype(F32)).astype(BF)
    outgoing = mark(jnp.dot(placing, embeds, preferred_element_type=F32).astype(BF))
    image_embeds = exchange(outgoing, everyone)

    in_low, in_high = mark(add_pair(in_terms, 0, go(*in_coming)))
    out_low, out_high = add_pair(out_terms, 0, go(*out_coming))
    low = jnp.concatenate([in_low, out_low], axis=1)
    high = jnp.concatenate([in_high, out_high], axis=1)
    low, high = lax.optimization_barrier((low, high))
    mark((low, high))

    def term(value, index, k):
        return pick(value, (index + way * k) % RING)

    arrived_low = (
        send(term(low, z, 1), "z"),
        send_across(term(low, z, 2), "z"),
        send(term(low, z, 3), "z", reverse=True),
    )
    arrived_high = (
        send(term(high, x, 1), "x"),
        send_across(term(high, x, 2), "x"),
        send(term(high, x, 3), "x", reverse=True),
    )

    grad_normed = plus(features[2], go(coming))
    scaled = grad_normed * gain
    projection = jnp.mean(scaled * merged, axis=-1, keepdims=True)
    cubed = inverse * inverse * inverse
    grad_patches = mark((inverse * scaled - merged * cubed * projection).astype(BF))

    def whole(own, arrived):
        return sum((piece.astype(F32) for piece in arrived), own.astype(F32)).astype(BF)

    arrived_low, arrived_high = go(arrived_low, arrived_high)
    low, high = whole(pick(low, z), arrived_low), whole(pick(high, x), arrived_high)
    other = swap(jnp.where(core == 0, high, low))
    own = jnp.where(core == 0, low, high)
    rows = jnp.where(
        core == 0,
        jnp.concatenate([own, other], axis=1),
        jnp.concatenate([other, own], axis=1),
    ).astype(F32)
    split = width // (2 * RING)
    return (image_embeds, rows[:split], rows[split:].T, grad_patches)


def solution(mesh):
    grid = Mesh(mesh.devices.reshape(RING, RING, 2, RING), ("z", "x", "c", "y"))
    enc = ("z", "x", "c")
    everyone = (*enc, "y")
    in_specs = (
        P(enc, "y"),
        P(),
        P(None, "y"),
        P("y"),
        P("y", None),
        P(),
        P(everyone, None),
        P(everyone, None),
    )
    out_specs = (P(everyone, None), P(enc, "y"), P("y", enc), P(enc, "y"))

    return jax.shard_map(
        local, mesh=grid, in_specs=in_specs, out_specs=out_specs, check_vma=False
    )
```

```python
import jax
import jax.numpy as jnp
from jax import lax
from jax.experimental import pallas as pl
from jax.experimental.pallas import tpu as pltpu
from jax.sharding import Mesh
from jax.sharding import PartitionSpec as P


EPSILON = 1e-06
HALF_ROOT = 0.7071067811865476
DENSITY = 0.3989422804014327
RING = 4
BF = jnp.bfloat16
F32 = jnp.float32


def send(value, axis, reverse=False):
    pairs = []
    for place in range(RING):
        for core in range(2):
            to = (place + (1 - 2 * core) * (-1 if reverse else 1)) % RING
            if axis == "y":
                pairs.append((core * RING + place, core * RING + to))
            else:
                pairs.append((2 * place + core, 2 * to + core))
    return lax.ppermute(value, ("c", "y") if axis == "y" else (axis, "c"), pairs)


def send_across(value, axis):
    return lax.ppermute(value, axis, [(i, (i + 2) % RING) for i in range(RING)])


def swap(value):
    return lax.ppermute(value, "c", [(0, 1), (1, 0)])


def exchange(value, axis):
    return lax.all_to_all(value, axis, 0, 0, tiled=True)


def pick(stacked, index):
    return lax.dynamic_index_in_dim(stacked, index, 0, keepdims=False)


def t_dot(left, right):
    return lax.dot_general(left, right, (((0,), (0,)), ((), ())), preferred_element_type=F32)


def dot_t(left, right):
    return lax.dot_general(left, right, (((1,), (1,)), ((), ())), preferred_element_type=F32)


def plus(first, second):
    return first.astype(F32) + second.astype(F32)


def total(pieces):
    return jnp.sum(pieces.astype(F32), axis=0)


def weight_kernel(where, own_left, other_left, own_right, other_right, low, high, low_start, high_start):
    rows = low.shape[2]
    width = RING * rows

    def one(i, carry):
        cut = pl.ds(pl.multiple_of(i * width, width), width)
        own, other = (
            left[0, :, cut] if len(left.shape) == 3 else left[:, cut]
            for left in (own_left, other_left)
        )
        term = t_dot(own, own_right[...]) + t_dot(other, other_right[...])
        for x in range(2):
            start = 2 * rows * x
            low[2 * i + x, 0] = term[start : start + rows].astype(BF)
            high[0, 2 * i + x] = term[start + rows : start + 2 * rows].astype(BF)
        return carry

    lax.fori_loop(0, 2, one, 0)
    low_start[0] = low[where[0], 0]

    @pl.when(pl.program_id(0) == where[1])
    def _():
        high_start[...] = high[0]


def weight_terms(starts, own_left, other_left, own_right, other_right):
    tokens = own_left.shape[-2]
    columns = own_right.shape[1]
    if own_left.ndim == 3:
        width = own_left.shape[2]
        left = pl.BlockSpec((1, tokens, width), lambda z, where: (z, 0, 0))
    else:
        width = own_left.shape[1] // RING
        left = pl.BlockSpec((tokens, width), lambda z, where: (0, z))
    rows = width // (2 * RING)
    right = pl.BlockSpec((tokens, columns), lambda z, where: (0, 0))
    whole = jax.ShapeDtypeStruct((RING, RING, rows, columns), BF)
    first = jax.ShapeDtypeStruct((RING, rows, columns), BF)
    return pl.pallas_call(
        weight_kernel,
        grid_spec=pltpu.PrefetchScalarGridSpec(
            num_scalar_prefetch=1,
            grid=(RING,),
            in_specs=[left, left, right, right],
            out_specs=[
                pl.BlockSpec((RING, 1, rows, columns), lambda z, where: (0, z, 0, 0)),
                pl.BlockSpec((1, RING, rows, columns), lambda z, where: (z, 0, 0, 0)),
                pl.BlockSpec((1, rows, columns), lambda z, where: (z, 0, 0)),
                pl.BlockSpec((RING, rows, columns), lambda z, where: (0, 0, 0)),
            ],
        ),
        out_shape=[whole, whole, first, first],
        cost_estimate=cost(4 * RING * tokens * width * columns, 20_000_000),
    )(jnp.stack(starts), own_left, other_left, own_right, other_right)


def cost(flops, moved):
    return pl.CostEstimate(flops=flops, bytes_accessed=moved, transcendentals=0)


def hidden_kernel(where, part, weights, *refs):
    *earlier, out, filed = refs
    held = earlier[0]
    rows = part.shape[0] // 4

    def one(i, carry):
        cut = pl.ds(pl.multiple_of(i * rows, rows), rows)
        term = jnp.dot(part[cut], weights[0], preferred_element_type=F32)
        out[cut] = term + (held[...] if held.shape[0] == 1 else held[cut]).astype(F32)
        return carry

    lax.fori_loop(0, 4, one, 0)

    @pl.when(pl.program_id(0) == 0)
    def _():
        filed[0] = part[...]


def hidden_terms(block, part, weights, held, filed):
    tokens, width = part.shape
    units = weights.shape[2]
    cut = units // 2
    first = filed is None
    return pl.pallas_call(
        hidden_kernel,
        grid_spec=pltpu.PrefetchScalarGridSpec(
            num_scalar_prefetch=1,
            grid=(2,),
            in_specs=[
                pl.BlockSpec((tokens, width), lambda i, where: (0, 0)),
                pl.BlockSpec((1, width, cut), lambda i, where: (where[0], 0, i)),
                pl.BlockSpec((1 if first else tokens, cut), lambda i, where: (0, i)),
                *([] if first else [pl.BlockSpec(memory_space=pl.ANY)]),
            ],
            out_specs=[
                pl.BlockSpec((tokens, cut), lambda i, where: (0, i)),
                pl.BlockSpec((1, tokens, width), lambda i, where: (where[0], 0, 0)),
            ],
        ),
        out_shape=[
            jax.ShapeDtypeStruct((tokens, units), F32),
            jax.ShapeDtypeStruct((RING, tokens, width), BF),
        ],
        input_output_aliases={} if first else {4: 1},
        cost_estimate=cost(2 * tokens * width * units, 10_000_000),
    )(jnp.stack([block]), part, weights, held, *([] if first else [filed]))


def local(patches, ln_gain, w_in, b_in, w_out, b_out, owner, cotangent):
    z, x, core, y = (lax.axis_index(name) for name in ("z", "x", "c", "y"))
    way = 1 - 2 * core
    everyone = ("z", "x", "c", "y")
    devices = lax.axis_size(everyone)
    slot_cap = cotangent.shape[0] // devices
    tokens, width = patches.shape
    own_rows = tokens // RING
    gain = ln_gain.astype(F32)
    last = owner

    def send_all(in_pair, out_pair):
        low, high, out_low, out_high = lax.optimization_barrier((*in_pair, *out_pair))
        return (
            (send(low, "x"), send(high, "z")),
            (send(out_low, "x"), send(out_high, "z")),
        )

    def add_pair(terms, k, arrived):
        low = pick(terms[0], (x + way * k) % RING).astype(F32) + arrived[0].astype(F32)
        high = pick(terms[1], (z + way * k) % RING).astype(F32) + arrived[1].astype(F32)
        return low.astype(BF), high.astype(BF)

    def go(*values):
        out = lax.optimization_barrier((*values, last))[:-1]
        return out if len(out) > 1 else out[0]

    def mark(value):
        nonlocal last
        last = value
        return value

    def place(places):
        return (y + way * places) % RING

    targets = owner[:, 0]
    before = jnp.arange(own_rows)[:, None] > jnp.arange(own_rows)[None, :]
    same_owner = targets[:, None] == targets[None, :]
    rank_in = jnp.sum(jnp.logical_and(same_owner, before), axis=1)
    slot_ids = targets * slot_cap + rank_in
    placing = (
        jnp.arange(devices * slot_cap, dtype=jnp.int32)[:, None] == slot_ids[None, :]
    ).astype(BF)

    merged = patches.astype(F32)
    inverse = lax.rsqrt(jnp.mean(merged * merged, axis=-1, keepdims=True) + EPSILON)
    part = mark((merged * inverse * gain).astype(BF))
    coming = send(part, "y")
    returned = exchange(go(cotangent), everyone)

    w_in_blocks = w_in.reshape(RING, width, -1)
    hidden, normed = mark(
        hidden_terms(place(0), go(part), w_in_blocks, b_in[None], None)
    )
    part = go(coming)
    coming = send(part, "y")
    hidden, normed = mark(hidden_terms(place(-1), part, w_in_blocks, hidden, normed))
    part_grad = mark(t_dot(placing, go(returned)).astype(BF))
    coming_grad = send(part_grad, "y")
    grad_embeds = jnp.zeros((RING, *part_grad.shape), BF)
    grad_embeds = lax.dynamic_update_index_in_dim(grad_embeds, part_grad, y, 0)
    part = mark(go(coming))
    coming = send(part, "y")
    hidden, normed = mark(hidden_terms(place(-2), part, w_in_blocks, hidden, normed))
    part_grad = mark(go(coming_grad))
    coming_grad = send(part_grad, "y")
    grad_embeds = lax.dynamic_update_index_in_dim(grad_embeds, part_grad, place(-1), 0)
    part = mark(go(coming))
    normed = lax.dynamic_update_index_in_dim(normed, part, place(-3), 0)
    hidden = hidden + jnp.dot(
        part, pick(w_in_blocks, place(-3)), preferred_element_type=F32
    )
    other_normed = swap(normed)
    cdf = 0.5 * (1.0 + lax.erf(hidden * HALF_ROOT))
    active = mark((hidden * cdf).astype(BF))
    slope = cdf + hidden * jnp.exp(-0.5 * hidden * hidden) * DENSITY

    part_grad = mark(go(coming_grad))
    coming_grad = send(part_grad, "y")
    grad_embeds = lax.dynamic_update_index_in_dim(grad_embeds, part_grad, place(-2), 0)
    partial = jnp.dot(go(active), w_out, preferred_element_type=F32).astype(BF)
    mark(partial)
    pieces = exchange(partial.reshape(RING, own_rows, -1), "y")
    half = active.shape[1] // 2

    def own_half(value, which):
        return lax.dynamic_slice_in_dim(value, which * half, half, 1)

    grad_embeds = lax.dynamic_update_index_in_dim(grad_embeds, go(coming_grad), place(-3), 0)
    grad_embeds = grad_embeds.reshape(tokens, -1)
    other_embeds = swap(grad_embeds)
    grad_hidden = (dot_t(grad_embeds, w_out) * slope).astype(BF)
    mark(grad_hidden)
    own_hidden, own_active = own_half(grad_hidden, core), own_half(active, core)
    other_hidden = swap(own_half(grad_hidden, 1 - core))
    other_active = swap(own_half(active, 1 - core))

    def feature_term(k, hidden_now, arrived=None):
        term = dot_t(hidden_now, pick(w_in_blocks, place(k)))
        return (term if arrived is None else term + arrived.astype(F32)).astype(BF)

    held = mark(feature_term(3, go(grad_hidden)))
    coming = send(held, "y")

    starts = [(x + way * 3) % RING, (z + way * 3) % RING]
    *out_terms, low, high = mark(
        weight_terms(starts, *go(grad_embeds, other_embeds, own_active, other_active))
    )
    out_held = low, high
    *in_terms, low, high = mark(
        weight_terms(starts, *go(normed, other_normed, own_hidden, other_hidden))
    )
    in_coming, out_coming = send_all((low, high), out_held)

    held = mark(feature_term(2, *go(grad_hidden, coming)))
    coming = send(held, "y")
    embeds = (total(go(pieces)) + b_out.astype(F32)).astype(BF)
    outgoing = mark(jnp.dot(placing, embeds, preferred_element_type=F32).astype(BF))
    image_embeds = exchange(outgoing, everyone)

    in_held = mark(add_pair(in_terms, 2, go(*in_coming)))
    out_held = mark(add_pair(out_terms, 2, go(*out_coming)))
    in_coming, out_coming = send_all(in_held, out_held)

    held = mark(feature_term(1, *go(grad_hidden, coming)))
    coming = send(held, "y")
    feature = mark(feature_term(0, go(grad_hidden)))

    in_held = mark(add_pair(in_terms, 1, go(*in_coming)))
    out_held = mark(add_pair(out_terms, 1, go(*out_coming)))
    in_coming, out_coming = send_all(in_held, out_held)

    grad_normed = plus(feature, go(coming))
    scaled = grad_normed * gain
    projection = jnp.mean(scaled * merged, axis=-1, keepdims=True)
    cubed = inverse * inverse * inverse
    grad_patches = mark((inverse * scaled - merged * cubed * projection).astype(BF))

    in_low, in_high = mark(add_pair(in_terms, 0, go(*in_coming)))
    out_low, out_high = add_pair(out_terms, 0, go(*out_coming))
    low = jnp.concatenate([in_low, out_low], axis=1)
    high = jnp.concatenate([in_high, out_high], axis=1)
    low, high = lax.optimization_barrier((low, high))
    mark((low, high))

    def term(value, index, k):
        return pick(value, (index + way * k) % RING)

    arrived_low = (
        send(term(low, z, 1), "z"),
        send_across(term(low, z, 2), "z"),
        send(term(low, z, 3), "z", reverse=True),
    )
    arrived_high = (
        send(term(high, x, 1), "x"),
        send_across(term(high, x, 2), "x"),
        send(term(high, x, 3), "x", reverse=True),
    )

    def whole(own, arrived):
        return sum((piece.astype(F32) for piece in arrived), own.astype(F32)).astype(BF)

    arrived_low, arrived_high = go(arrived_low, arrived_high)
    low, high = whole(pick(low, z), arrived_low), whole(pick(high, x), arrived_high)
    other = swap(jnp.where(core == 0, high, low))
    own = jnp.where(core == 0, low, high)
    rows = jnp.where(
        core == 0,
        jnp.concatenate([own, other], axis=1),
        jnp.concatenate([other, own], axis=1),
    ).astype(F32)
    split = width // (2 * RING)
    return (image_embeds, rows[:split], rows[split:].T, grad_patches)


def solution(mesh):
    grid = Mesh(mesh.devices.reshape(RING, RING, 2, RING), ("z", "x", "c", "y"))
    enc = ("z", "x", "c")
    everyone = (*enc, "y")
    in_specs = (
        P(enc, "y"),
        P(),
        P(None, "y"),
        P("y"),
        P("y", None),
        P(),
        P(everyone, None),
        P(everyone, None),
    )
    out_specs = (P(everyone, None), P(enc, "y"), P("y", enc), P(enc, "y"))

    return jax.shard_map(
        local, mesh=grid, in_specs=in_specs, out_specs=out_specs, check_vma=False
    )
```

```python
import jax
import jax.numpy as jnp
from jax import lax
from jax.experimental import pallas as pl
from jax.experimental.pallas import tpu as pltpu
from jax.sharding import Mesh
from jax.sharding import PartitionSpec as P


EPSILON = 1e-06
HALF_ROOT = 0.7071067811865476
DENSITY = 0.3989422804014327
RING = 4
BF = jnp.bfloat16
F32 = jnp.float32


def send(value, axis, reverse=False):
    pairs = []
    for place in range(RING):
        for core in range(2):
            to = (place + (1 - 2 * core) * (-1 if reverse else 1)) % RING
            if axis == "y":
                pairs.append((core * RING + place, core * RING + to))
            else:
                pairs.append((2 * place + core, 2 * to + core))
    return lax.ppermute(value, ("c", "y") if axis == "y" else (axis, "c"), pairs)


def send_across(value, axis):
    return lax.ppermute(value, axis, [(i, (i + 2) % RING) for i in range(RING)])


def swap(value):
    return lax.ppermute(value, "c", [(0, 1), (1, 0)])


def exchange(value, axis):
    return lax.all_to_all(value, axis, 0, 0, tiled=True)


def pick(stacked, index):
    return lax.dynamic_index_in_dim(stacked, index, 0, keepdims=False)


def t_dot(left, right):
    return lax.dot_general(left, right, (((0,), (0,)), ((), ())), preferred_element_type=F32)


def dot_t(left, right):
    return lax.dot_general(left, right, (((1,), (1,)), ((), ())), preferred_element_type=F32)


def plus(first, second):
    return first.astype(F32) + second.astype(F32)


def total(pieces):
    return jnp.sum(pieces.astype(F32), axis=0)


def weight_kernel(where, own_left, other_left, own_right, other_right, low, high, low_start, high_start):
    rows = low.shape[2]
    width = RING * rows

    def one(i, carry):
        cut = pl.ds(pl.multiple_of(i * width, width), width)
        own, other = (
            left[0, :, cut] if len(left.shape) == 3 else left[:, cut]
            for left in (own_left, other_left)
        )
        term = t_dot(own, own_right[...]) + t_dot(other, other_right[...])
        for x in range(2):
            start = 2 * rows * x
            low[2 * i + x, 0] = term[start : start + rows].astype(BF)
            high[0, 2 * i + x] = term[start + rows : start + 2 * rows].astype(BF)
        return carry

    lax.fori_loop(0, 2, one, 0)
    low_start[0] = low[where[0], 0]

    @pl.when(pl.program_id(0) == where[1])
    def _():
        high_start[...] = high[0]


def weight_terms(starts, own_left, other_left, own_right, other_right):
    tokens = own_left.shape[-2]
    columns = own_right.shape[1]
    if own_left.ndim == 3:
        width = own_left.shape[2]
        left = pl.BlockSpec((1, tokens, width), lambda z, where: (z, 0, 0))
    else:
        width = own_left.shape[1] // RING
        left = pl.BlockSpec((tokens, width), lambda z, where: (0, z))
    rows = width // (2 * RING)
    right = pl.BlockSpec((tokens, columns), lambda z, where: (0, 0))
    whole = jax.ShapeDtypeStruct((RING, RING, rows, columns), BF)
    first = jax.ShapeDtypeStruct((RING, rows, columns), BF)
    return pl.pallas_call(
        weight_kernel,
        grid_spec=pltpu.PrefetchScalarGridSpec(
            num_scalar_prefetch=1,
            grid=(RING,),
            in_specs=[left, left, right, right],
            out_specs=[
                pl.BlockSpec((RING, 1, rows, columns), lambda z, where: (0, z, 0, 0)),
                pl.BlockSpec((1, RING, rows, columns), lambda z, where: (z, 0, 0, 0)),
                pl.BlockSpec((1, rows, columns), lambda z, where: (z, 0, 0)),
                pl.BlockSpec((RING, rows, columns), lambda z, where: (0, 0, 0)),
            ],
        ),
        out_shape=[whole, whole, first, first],
        cost_estimate=cost(4 * RING * tokens * width * columns, 20_000_000),
    )(jnp.stack(starts), own_left, other_left, own_right, other_right)


def cost(flops, moved):
    return pl.CostEstimate(flops=flops, bytes_accessed=moved, transcendentals=0)


def hidden_kernel(where, part, weights, *refs):
    *earlier, out, filed = refs
    term = jnp.dot(part[...], weights[0], preferred_element_type=F32)
    out[...] = term + earlier[0][...].astype(F32)

    @pl.when(pl.program_id(0) == 0)
    def _():
        filed[0] = part[...]


def hidden_terms(block, part, weights, held, filed):
    tokens, width = part.shape
    units = weights.shape[2]
    cut = units // 2
    first = filed is None
    return pl.pallas_call(
        hidden_kernel,
        grid_spec=pltpu.PrefetchScalarGridSpec(
            num_scalar_prefetch=1,
            grid=(2,),
            in_specs=[
                pl.BlockSpec((tokens, width), lambda i, where: (0, 0)),
                pl.BlockSpec((1, width, cut), lambda i, where: (where[0], 0, i)),
                pl.BlockSpec((1 if first else tokens, cut), lambda i, where: (0, i)),
                *([] if first else [pl.BlockSpec(memory_space=pl.ANY)]),
            ],
            out_specs=[
                pl.BlockSpec((tokens, cut), lambda i, where: (0, i)),
                pl.BlockSpec((1, tokens, width), lambda i, where: (where[0], 0, 0)),
            ],
        ),
        out_shape=[
            jax.ShapeDtypeStruct((tokens, units), F32),
            jax.ShapeDtypeStruct((RING, tokens, width), BF),
        ],
        input_output_aliases={} if first else {4: 1},
        cost_estimate=cost(2 * tokens * width * units, 10_000_000),
    )(jnp.stack([block]), part, weights, held, *([] if first else [filed]))


def local(patches, ln_gain, w_in, b_in, w_out, b_out, owner, cotangent):
    z, x, core, y = (lax.axis_index(name) for name in ("z", "x", "c", "y"))
    way = 1 - 2 * core
    everyone = ("z", "x", "c", "y")
    devices = lax.axis_size(everyone)
    slot_cap = cotangent.shape[0] // devices
    tokens, width = patches.shape
    own_rows = tokens // RING
    gain = ln_gain.astype(F32)
    last = owner

    def send_all(in_pair, out_pair):
        low, high, out_low, out_high = lax.optimization_barrier((*in_pair, *out_pair))
        return (
            (send(low, "x"), send(high, "z")),
            (send(out_low, "x"), send(out_high, "z")),
        )

    def add_pair(terms, k, arrived):
        low = pick(terms[0], (x + way * k) % RING).astype(F32) + arrived[0].astype(F32)
        high = pick(terms[1], (z + way * k) % RING).astype(F32) + arrived[1].astype(F32)
        return low.astype(BF), high.astype(BF)

    def go(*values):
        out = lax.optimization_barrier((*values, last))[:-1]
        return out if len(out) > 1 else out[0]

    def mark(value):
        nonlocal last
        last = value
        return value

    def place(places):
        return (y + way * places) % RING

    targets = owner[:, 0]
    before = jnp.arange(own_rows)[:, None] > jnp.arange(own_rows)[None, :]
    same_owner = targets[:, None] == targets[None, :]
    rank_in = jnp.sum(jnp.logical_and(same_owner, before), axis=1)
    slot_ids = targets * slot_cap + rank_in
    placing = (
        jnp.arange(devices * slot_cap, dtype=jnp.int32)[:, None] == slot_ids[None, :]
    ).astype(BF)

    merged = patches.astype(F32)
    inverse = lax.rsqrt(jnp.mean(merged * merged, axis=-1, keepdims=True) + EPSILON)
    part = mark((merged * inverse * gain).astype(BF))
    coming = send(part, "y")
    returned = exchange(go(cotangent), everyone)

    w_in_blocks = w_in.reshape(RING, width, -1)
    hidden, normed = mark(
        hidden_terms(place(0), go(part), w_in_blocks, b_in[None], None)
    )
    part = go(coming)
    coming = send(part, "y")
    hidden, normed = mark(hidden_terms(place(-1), part, w_in_blocks, hidden, normed))
    part_grad = mark(t_dot(placing, go(returned)).astype(BF))
    coming_grad = send(part_grad, "y")
    grad_embeds = jnp.zeros((RING, *part_grad.shape), BF)
    grad_embeds = lax.dynamic_update_index_in_dim(grad_embeds, part_grad, y, 0)
    part = mark(go(coming))
    coming = send(part, "y")
    part_grad = mark(go(coming_grad))
    coming_grad = send(part_grad, "y")
    grad_embeds = lax.dynamic_update_index_in_dim(grad_embeds, part_grad, place(-1), 0)
    hidden, normed = mark(
        hidden_terms(place(-2), go(part), w_in_blocks, hidden, normed)
    )
    part_grad = mark(go(coming_grad))
    coming_grad = send(part_grad, "y")
    grad_embeds = lax.dynamic_update_index_in_dim(grad_embeds, part_grad, place(-2), 0)
    mark(grad_embeds)
    part = go(coming)
    normed = lax.dynamic_update_index_in_dim(normed, part, place(-3), 0)
    hidden = hidden + jnp.dot(
        part, pick(w_in_blocks, place(-3)), preferred_element_type=F32
    )
    cdf = 0.5 * (1.0 + lax.erf(hidden * HALF_ROOT))
    active = mark((hidden * cdf).astype(BF))
    slope = cdf + hidden * jnp.exp(-0.5 * hidden * hidden) * DENSITY

    other_normed = swap(go(normed))
    half = active.shape[1] // 2

    def own_half(value, which):
        return lax.dynamic_slice_in_dim(value, which * half, half, 1)

    grad_embeds = lax.dynamic_update_index_in_dim(grad_embeds, go(coming_grad), place(-3), 0)
    grad_embeds = grad_embeds.reshape(tokens, -1)
    other_embeds = swap(grad_embeds)
    grad_hidden = mark((dot_t(grad_embeds, w_out) * slope).astype(BF))
    own_hidden, own_active = own_half(grad_hidden, core), own_half(active, core)
    other_hidden = swap(own_half(grad_hidden, 1 - core))
    other_active = swap(own_half(active, 1 - core))

    def feature_term(k, hidden_now, arrived=None):
        term = dot_t(hidden_now, pick(w_in_blocks, place(k)))
        return (term if arrived is None else term + arrived.astype(F32)).astype(BF)

    held = mark(feature_term(3, go(grad_hidden)))
    coming = send(held, "y")

    starts = [(x + way * 3) % RING, (z + way * 3) % RING]
    *out_terms, low, high = mark(
        weight_terms(starts, *go(grad_embeds, other_embeds, own_active, other_active))
    )
    out_held = low, high
    *in_terms, low, high = mark(
        weight_terms(starts, *go(normed, other_normed, own_hidden, other_hidden))
    )
    in_coming, out_coming = send_all((low, high), out_held)

    held = mark(feature_term(2, *go(grad_hidden, coming)))
    coming = send(held, "y")
    partial = mark(jnp.dot(go(active), w_out, preferred_element_type=F32).astype(BF))
    pieces = exchange(partial.reshape(RING, own_rows, -1), "y")

    in_held = mark(add_pair(in_terms, 2, go(*in_coming)))
    out_held = mark(add_pair(out_terms, 2, go(*out_coming)))
    in_coming, out_coming = send_all(in_held, out_held)

    held = mark(feature_term(1, *go(grad_hidden, coming)))
    coming = send(held, "y")
    feature = mark(feature_term(0, go(grad_hidden)))

    in_held = mark(add_pair(in_terms, 1, go(*in_coming)))
    out_held = mark(add_pair(out_terms, 1, go(*out_coming)))
    in_coming, out_coming = send_all(in_held, out_held)

    embeds = (total(go(pieces)) + b_out.astype(F32)).astype(BF)
    outgoing = mark(jnp.dot(placing, embeds, preferred_element_type=F32).astype(BF))
    image_embeds = exchange(outgoing, everyone)

    in_low, in_high = mark(add_pair(in_terms, 0, go(*in_coming)))
    out_low, out_high = add_pair(out_terms, 0, go(*out_coming))
    low = jnp.concatenate([in_low, out_low], axis=1)
    high = jnp.concatenate([in_high, out_high], axis=1)
    low, high = lax.optimization_barrier((low, high))
    mark((low, high))

    def term(value, index, k):
        return pick(value, (index + way * k) % RING)

    arrived_low = (
        send(term(low, z, 1), "z"),
        send_across(term(low, z, 2), "z"),
        send(term(low, z, 3), "z", reverse=True),
    )
    arrived_high = (
        send(term(high, x, 1), "x"),
        send_across(term(high, x, 2), "x"),
        send(term(high, x, 3), "x", reverse=True),
    )

    grad_normed = plus(feature, go(coming))
    scaled = grad_normed * gain
    projection = jnp.mean(scaled * merged, axis=-1, keepdims=True)
    cubed = inverse * inverse * inverse
    grad_patches = mark((inverse * scaled - merged * cubed * projection).astype(BF))

    def whole(own, arrived):
        return sum((piece.astype(F32) for piece in arrived), own.astype(F32)).astype(BF)

    arrived_low, arrived_high = go(arrived_low, arrived_high)
    low, high = whole(pick(low, z), arrived_low), whole(pick(high, x), arrived_high)
    other = swap(jnp.where(core == 0, high, low))
    own = jnp.where(core == 0, low, high)
    rows = jnp.where(
        core == 0,
        jnp.concatenate([own, other], axis=1),
        jnp.concatenate([other, own], axis=1),
    ).astype(F32)
    split = width // (2 * RING)
    return (image_embeds, rows[:split], rows[split:].T, grad_patches)


def solution(mesh):
    grid = Mesh(mesh.devices.reshape(RING, RING, 2, RING), ("z", "x", "c", "y"))
    enc = ("z", "x", "c")
    everyone = (*enc, "y")
    in_specs = (
        P(enc, "y"),
        P(),
        P(None, "y"),
        P("y"),
        P("y", None),
        P(),
        P(everyone, None),
        P(everyone, None),
    )
    out_specs = (P(everyone, None), P(enc, "y"), P("y", enc), P(enc, "y"))

    return jax.shard_map(
        local, mesh=grid, in_specs=in_specs, out_specs=out_specs, check_vma=False
    )
```
